32 devices in a mesh: vocab: 4 (over x, core), section: 2 (over y), dp: 4 (over z).
Axes of the slice: x: 2, y: 2, z: 4, core: 2. Of those that a mesh axis runs over, the one named last changes fastest.
Arguments:
- teacher_hidden: bfloat16 [128, 16384], P(('dp', 'vocab', 'section')), parts along dimension 0, may hold values from -12 to 12
- student_hidden: bfloat16 [128, 8192], P(('dp', 'vocab', 'section')), parts along dimension 0, may hold values from -12 to 12
- teacher_head: bfloat16 [16384, 2048], P(None, ('vocab', 'section')), may hold values from -0.051452637 to 0.051452637
- student_head: bfloat16 [8192, 2048], P(None, ('vocab', 'section')), may hold values from -0.07544653 to 0.07544653
- token_weight: float32 [128], P('dp'), parts along dimension 0, may hold values from 1 to 30
Outputs:
- token_kl: float32 [128], P(('dp', 'vocab', 'section')), parts along dimension 0
- hidden_grad: float32 [128, 8192], P(('dp', 'vocab', 'section')), parts along dimension 0
The draws below stay inside these ranges and needn't reach their ends.
There are 4 independent parts, one for each index of `dp`. The reference program is written for one: setup_inputs(seed, part) draws one part's arguments, and reference() takes and returns one part's arrays. A program takes and returns all parts, laid end to end along the dimension named above; an argument that names none is the same for every part. Nothing has to cross between parts.
All inputs are finite; a program needn't handle non-finite values.
Results may differ from the reference program's by a relative error of at most 0.0042.
Values may be sent and summed in bfloat16 or wider, within the bound.
A program may use at most 128 MiB of HBM per device.

```python
import math
import jax
import jax.numpy as jnp
from jax import lax

DT = 16384
DS = 8192
TOKENS = 32
VOCAB = 2048


direction_count = 8


def walsh_signs(width):
    index = jnp.arange(width, dtype=jnp.int32)
    masks = (jnp.arange(direction_count, dtype=jnp.int32) + 1) * 2731 % width
    parity = jnp.bitwise_and(index[None, :], masks[:, None])
    for shift in (16, 8, 4, 2, 1):
        parity = jnp.bitwise_xor(parity, jnp.right_shift(parity, shift))
    return 1.0 - 2.0 * jnp.bitwise_and(parity, 1).astype(jnp.float32)


def planted_columns(key, salt):
    order = jax.random.permutation(jax.random.fold_in(key, 71), VOCAB)
    first = order[:direction_count]
    second = order[direction_count:2 * direction_count]
    strength = 55.0 + 20.0 * jax.random.uniform(jax.random.fold_in(key, salt), (direction_count,), jnp.float32)
    strength = strength.at[0].set(75.0)
    spacing = 0.5 + 0.25 * jax.random.uniform(jax.random.fold_in(key, salt + 1), (direction_count,), jnp.float32)
    return (first, second, strength, spacing)


def planted_head(key, width, salt):
    scale = width ** (-0.5)
    noise = jax.random.normal(jax.random.fold_in(key, salt + 2), (width, VOCAB), jnp.float32)
    base = jnp.clip(scale * noise, -6.0 * scale, 6.0 * scale)
    first, second, strength, spacing = planted_columns(key, salt)
    signs = walsh_signs(width).T
    shared = base[:, first]
    base = base.at[:, first].set(shared + signs * (strength / width)[None, :])
    base = base.at[:, second].set(shared + signs * ((strength - spacing) / width)[None, :])
    return base.astype(jnp.bfloat16)


def planted_tokens(key):
    count = max(2, TOKENS // 16)
    chosen = jax.random.permutation(jax.random.fold_in(key, 81), TOKENS)[:count]
    direction = jax.random.randint(jax.random.fold_in(key, 82), (count,), 0, direction_count)
    direction = direction.at[0].set(0)
    return (chosen, direction)


def planted_hidden(key, width, salt):
    shape = (TOKENS, width)
    base = jnp.clip(3.0 * jax.random.normal(jax.random.fold_in(key, salt + 1), shape, jnp.float32), -8.0, 8.0)
    chosen, direction = planted_tokens(key)
    level = 2.0 + 2.0 * jax.random.uniform(jax.random.fold_in(key, salt + 2), (chosen.shape[0],), jnp.float32)
    level = level.at[0].set(4.0)
    signs = walsh_signs(width)[direction]
    base = base.at[chosen].add(level[:, None] * signs)
    return base.astype(jnp.bfloat16)


def draw_teacher_hidden(key, part):
    return planted_hidden(key, DT, 11)


def draw_student_hidden(key, part):
    return planted_hidden(key, DS, 21)


def draw_teacher_head(key, part):
    return planted_head(key, DT, 31)


def draw_student_head(key, part):
    return planted_head(key, DS, 41)


def setup_inputs(seed: int = 0, part: int = 0) -> dict:
    key_list = jax.random.split(jax.random.key(seed), 6)
    part_splits = jax.random.split(jax.random.fold_in(key_list[5], part), 6)
    return {
        "teacher_hidden": draw_teacher_hidden(jax.random.fold_in(jax.random.fold_in(key_list[5], part), 71), part),
        "student_hidden": draw_student_hidden(jax.random.fold_in(jax.random.fold_in(key_list[5], part), 71), part),
        "teacher_head": draw_teacher_head(jax.random.fold_in(key_list[5], 71), part),
        "student_head": draw_student_head(jax.random.fold_in(key_list[5], 71), part),
        "token_weight": jnp.clip(jnp.exp(jax.random.uniform(part_splits[4], (TOKENS,), jnp.float32, math.log(1.0), math.log(30.0))), 1.0, 30.0),
    }


def reference(teacher_hidden, student_hidden, teacher_head, student_head, token_weight):
    teacher_logits = jnp.dot(teacher_hidden, teacher_head, preferred_element_type=jnp.float32)
    student_logits = jnp.dot(student_hidden, student_head, preferred_element_type=jnp.float32)
    teacher_max = jnp.max(teacher_logits, axis=1)
    student_max = jnp.max(student_logits, axis=1)
    teacher_exp = jnp.exp(teacher_logits - teacher_max[:, None])
    teacher_total = jnp.sum(teacher_exp, axis=1)
    student_total = jnp.sum(jnp.exp(student_logits - student_max[:, None]), axis=1)
    cross = jnp.sum(teacher_exp * (teacher_logits - student_logits), axis=1)
    teacher_lse = teacher_max + jnp.log(teacher_total)
    student_lse = student_max + jnp.log(student_total)
    token_kl = cross / teacher_total - teacher_lse + student_lse
    diff = jnp.exp(student_logits - student_lse[:, None]) - jnp.exp(teacher_logits - teacher_lse[:, None])
    logit_grad = (token_weight[:, None] * diff).astype(jnp.bfloat16)
    hidden_grad = lax.dot_general(logit_grad, student_head, (((1,), (1,)), ((), ())), preferred_element_type=jnp.float32)
    return token_kl, hidden_grad
```

```python
import functools

import jax
import jax.numpy as jnp
from jax import lax
from jax.experimental import pallas as pl
from jax.experimental.pallas import tpu as pltpu
from jax.sharding import PartitionSpec as P

CORES = 2
PACK = 16
BLOCK = 8
F32 = jnp.float32


def kernel(
    dims,
    th_hbm,
    sh_hbm,
    tw_ref,
    thead_hbm,
    shead_hbm,
    kl_ref,
    grad_ref,
    th_in,
    sh_in,
    thead,
    shead,
    phead,
    gt,
    gs,
    acc_t,
    acc_s,
    logits,
    plogits,
    stats,
    part,
    sbuf,
    rbuf,
    fbuf,
    pbuf,
    in_sem,
    thead_sem,
    phead_sem,
    send_sem,
    piece_sem,
    pair_sem,
    logit_sem,
    stat_sem,
    red_sem,
    fin_sem,
):
    n1, n2, chunks, red_width = dims
    nchips = n1 * n2
    n = nchips * CORES
    rows, kt = th_in.shape
    ks = sh_in.shape[1]
    fold = PACK // rows
    tokens = n * rows
    pair_rows = CORES * rows
    half = ks // CORES
    width = stats.shape[2]

    position, s = lax.axis_index("vocab"), lax.axis_index("section")
    v, c = position // CORES, position % CORES
    other = 1 - c
    chip = v * n2 + s
    slot = chip * CORES + c

    def device(v, s, c):
        return {"vocab": v * CORES + c, "section": s}

    sends = []

    def push(src, dst, recv, target):
        copy = pltpu.make_async_remote_copy(
            src_ref=src,
            dst_ref=dst,
            send_sem=send_sem.at[len(sends)],
            recv_sem=recv,
            device_id=target,
            device_id_type=pl.DeviceIdType.MESH,
        )
        copy.start()
        sends.append(copy)

    def arrive(dst, recv):
        pltpu.make_async_remote_copy(
            src_ref=dst,
            dst_ref=dst,
            send_sem=send_sem.at[0],
            recv_sem=recv,
            device_id=device(v, s, other),
            device_id_type=pl.DeviceIdType.MESH,
        ).wait_recv()

    barrier = pltpu.get_barrier_semaphore()
    for dv in range(n1):
        for ds in range(n2):
            for dc in range(CORES):
                if dv or ds or dc:
                    pl.semaphore_signal(
                        barrier,
                        inc=1,
                        device_id=device((v + dv) % n1, (s + ds) % n2, (c + dc) % CORES),
                        device_id_type=pl.DeviceIdType.MESH,
                    )
    load_t = pltpu.make_async_copy(th_hbm, th_in, in_sem.at[0])
    load_s = pltpu.make_async_copy(sh_hbm, sh_in, in_sem.at[1])
    load_t.start()
    load_s.start()
    loads = {}
    for index, (is_teacher, first, size, _) in enumerate(chunks):
        src, dst = (thead_hbm, thead) if is_teacher else (shead_hbm, shead)
        depth = (kt if is_teacher else ks) // fold
        for q in range(fold):
            span = pl.ds(q * depth + first, size)
            copy = pltpu.make_async_copy(src.at[span], dst.at[span], thead_sem.at[index, q])
            copy.start()
            loads[index, q] = copy

    load_t.wait()
    load_s.wait()
    for src, dst in ((th_in, gt), (sh_in, gs)):
        depth = src.shape[1] // fold
        dst[slot] = jnp.concatenate(
            [src[:, q * depth : (q + 1) * depth] for q in range(fold)], axis=0
        )
    row = lax.broadcasted_iota(jnp.int32, (tokens, width), 0)
    lane = lax.broadcasted_iota(jnp.int32, (tokens, width), 1)
    eye = row == lane
    row_chip, row_core, row_token = row // pair_rows, row % pair_rows // rows, row % rows
    source = ((row_chip // n2 * CORES + row_core) * n2 + row_chip % n2) * rows + row_token
    weight = jnp.sum(
        jnp.where(source == lane, jnp.broadcast_to(tw_ref[...], (tokens, width)), 0.0),
        axis=1,
        keepdims=True,
    )
    pl.semaphore_wait(barrier, n - 1)

    def piece(index, where, h):
        is_teacher, first, size, _ = chunks[index]
        buf = gt if is_teacher else gs
        return buf.at[where, :, pl.ds(first + h * (size // 2), size // 2)]

    def whole(index, where):
        is_teacher, first, size, _ = chunks[index]
        buf = gt if is_teacher else gs
        return buf.at[where, :, pl.ds(first, size)]

    def slot_of(v, s, c):
        return (v * n2 + s) * CORES + c

    count = len(chunks)
    along_v = [(v + dv) % n1 for dv in range(1, n1)]
    along_s = [(s + ds) % n2 for ds in range(1, n2)]
    for i in range(count):
        for h in range(2):
            ref, sem = piece(i, slot, h), piece_sem.at[2 * i + h, slot]
            first = [device(to, s, c) for to in along_v]
            second = [device(v, to, c) for to in along_s]
            for target in first + second:
                push(ref, ref, sem, target)
        push(whole(i, slot), whole(i, slot), pair_sem.at[i, slot], device(v, s, other))
    push(
        shead_hbm.at[pl.ds(pl.multiple_of(other * half, half), half)],
        phead,
        phead_sem,
        device(v, s, other),
    )
    for i in range(count):
        for h in range(2):
            for frm in along_v:
                at = slot_of(frm, s, c)
                ref, sem = piece(i, at, h), piece_sem.at[2 * i + h, at]
                arrive(ref, sem)
                if h == 0:
                    for to in along_s:
                        push(ref, ref, sem, device(v, to, c))
            for frm in along_s:
                at = slot_of(v, frm, c)
                ref, sem = piece(i, at, h), piece_sem.at[2 * i + h, at]
                arrive(ref, sem)
                if h == 1:
                    for to in along_v:
                        push(ref, ref, sem, device(to, s, c))
        for at in [slot_of(frm, s, c) for frm in along_v] + [slot_of(v, frm, c) for frm in along_s]:
            push(whole(i, at), whole(i, at), pair_sem.at[i, at], device(v, s, other))

    block = min(BLOCK, n)
    row_part = lax.broadcasted_iota(jnp.int32, (block * PACK, acc_t.shape[1]), 0) % PACK // rows
    for i in range(count):
        for fv in along_v:
            for fs in along_s:
                at = slot_of(fv, fs, c)
                for h in range(2):
                    arrive(piece(i, at, h), piece_sem.at[2 * i + h, at])
                push(whole(i, at), whole(i, at), pair_sem.at[i, at], device(v, s, other))
        for fv in range(n1):
            for fs in range(n2):
                at = slot_of((v + fv) % n1, (s + fs) % n2, other)
                arrive(whole(i, at), pair_sem.at[i, at])
        for q in range(fold):
            loads[i, q].wait()
        is_teacher, first, size, fresh = chunks[i]
        buf, head, acc = (gt, thead, acc_t) if is_teacher else (gs, shead, acc_s)
        depth = (kt if is_teacher else ks) // fold

        def multiply(b):
            lhs = buf[pl.ds(b * block, block), :, first : first + size].reshape(block * PACK, size)
            total = None
            for q in range(fold):
                rhs = head[q * depth + first : q * depth + first + size, :]
                product = jnp.dot(lhs, rhs, preferred_element_type=F32)
                total = product if total is None else jnp.where(row_part == q, product, total)
            where = pl.ds(b * block * PACK, block * PACK)
            acc[where, :] = total if fresh else acc[where, :] + total

        if n > block:
            pl.loop(0, n // block)(multiply)
        else:
            multiply(0)

    def compact(acc):
        cols = acc.shape[1]
        x = acc[...].reshape(n, PACK // 8, 8, cols)
        total = x[:, 0] + x[:, 1]
        total = total + jnp.concatenate([total[:, rows:], total[:, :rows]], axis=1)
        total = total.reshape(nchips, CORES, 8, cols)
        sub = lax.broadcasted_iota(jnp.int32, (nchips, 8, cols), 1)
        return jnp.where(sub < rows, total[:, 0], total[:, 1]).reshape(tokens, cols)

    tl, sl = compact(acc_t), compact(acc_s)
    logits[0] = tl
    logits[1] = sl
    push(logits, plogits, logit_sem, device(v, s, other))
    tmax = jnp.max(tl, axis=1, keepdims=True)
    smax = jnp.max(sl, axis=1, keepdims=True)
    texp = jnp.exp(tl - tmax)
    columns = (
        tmax,
        smax,
        jnp.sum(texp, axis=1, keepdims=True),
        jnp.sum(jnp.exp(sl - smax), axis=1, keepdims=True),
        jnp.sum(texp * (tl - sl), axis=1, keepdims=True),
    )
    lines = [jnp.sum(jnp.where(eye, col, 0.0), axis=0, keepdims=True) for col in columns]
    lines.append(jnp.zeros((8 - len(lines), width), F32))
    stats[slot] = jnp.concatenate(lines, axis=0)
    for dv in reversed(range(n1)):
        for ds in reversed(range(n2)):
            for dc in range(CORES):
                if dv or ds or dc:
                    to = device((v + dv) % n1, (s + ds) % n2, (c + dc) % CORES)
                    push(stats.at[slot], stats.at[slot], stat_sem.at[slot], to)
    for dv in range(n1):
        for ds in range(n2):
            for dc in range(CORES):
                if dv or ds or dc:
                    at = slot_of((v + dv) % n1, (s + ds) % n2, (c + dc) % CORES)
                    arrive(stats.at[at], stat_sem.at[at])
    arrive(plogits, logit_sem)
    arrive(phead, phead_sem)
    allstats = stats[...]
    tm, sm = allstats[:, 0], allstats[:, 1]
    tmax = jnp.max(tm, axis=0, keepdims=True)
    smax = jnp.max(sm, axis=0, keepdims=True)
    tscale = jnp.exp(tm - tmax)
    ttotal = jnp.sum(allstats[:, 2] * tscale, axis=0, keepdims=True)
    stotal = jnp.sum(allstats[:, 3] * jnp.exp(sm - smax), axis=0, keepdims=True)
    cross = jnp.sum(allstats[:, 4] * tscale, axis=0, keepdims=True)
    tlse = tmax + jnp.log(ttotal)
    slse = smax + jnp.log(stotal)
    kl = cross / ttotal - tlse + slse

    def column(line):
        return jnp.sum(
            jnp.where(eye, jnp.broadcast_to(line, (tokens, width)), 0.0), axis=1, keepdims=True
        )

    tlse, slse = column(tlse), column(slse)
    grads = []
    for ref in (logits, plogits):
        diff = jnp.exp(ref[1] - slse) - jnp.exp(ref[0] - tlse)
        grads.append((weight * diff).astype(jnp.bfloat16))

    steps = half // red_width
    nt = (((1,), (1,)), ((), ()))
    for j in range(steps):
        mine = pl.ds(pl.multiple_of(c * half + j * red_width, red_width), red_width)
        total = lax.dot_general(grads[0], shead[mine, :], nt, preferred_element_type=F32)
        total += lax.dot_general(
            grads[1],
            phead[j * red_width : (j + 1) * red_width, :],
            nt,
            preferred_element_type=F32,
        )
        total = total.reshape(nchips, pair_rows, red_width)
        part[:, :, j * red_width : (j + 1) * red_width] = total
        packed = jnp.concatenate(
            [total[:, :, : red_width // 2], total[:, :, red_width // 2 :]], axis=1
        )
        sbuf[:, j] = packed.astype(jnp.bfloat16)
        for dv in reversed(range(n1)):
            for ds in reversed(range(n2)):
                if dv or ds:
                    tv, ts = (v + dv) % n1, (s + ds) % n2
                    push(
                        sbuf.at[tv * n2 + ts, j],
                        rbuf.at[chip, j],
                        red_sem.at[chip, j],
                        device(tv, ts, c),
                    )

    kl_rows = column(kl)
    kl_ref[...] = jnp.sum(jnp.where(row == slot * rows + lane, kl_rows, 0.0), axis=0, keepdims=True)[
        :, :rows
    ]

    def pick(value, which):
        return jnp.where(which == 0, value[:rows], value[rows:])

    for j in range(steps):
        total = part[chip, :, j * red_width : (j + 1) * red_width]
        for dv in range(n1):
            for ds in range(n2):
                if dv or ds:
                    at = (v + dv) % n1 * n2 + (s + ds) % n2
                    arrive(rbuf.at[at, j], red_sem.at[at, j])
                    got = rbuf[at, j].astype(F32)
                    total += jnp.concatenate([got[:pair_rows], got[pair_rows:]], axis=1)
        fbuf[j] = total
        push(fbuf.at[j], pbuf.at[j], fin_sem.at[j], device(v, s, other))
        to = pl.multiple_of(c * half + j * red_width, red_width)
        grad_ref[:, pl.ds(to, red_width)] = pick(total, c)
    for j in range(steps):
        arrive(pbuf.at[j], fin_sem.at[j])
        to = pl.multiple_of(other * half + j * red_width, red_width)
        grad_ref[:, pl.ds(to, red_width)] = pick(pbuf[j], c)
    for copy in sends:
        copy.wait_send()


def shards(n1, n2, th, sh, thead, shead, tw):
    nchips = n1 * n2
    n = nchips * CORES
    rows, kt = th.shape
    ks = sh.shape[1]
    cols = thead.shape[1]
    fold = PACK // rows
    tokens = n * rows
    width = -(-tokens // 128) * 128
    td, sd = kt // fold, ks // fold
    chunks = (
        (True, 0, td // 2, True),
        (True, td // 2, td // 2, False),
        (False, 0, sd, True),
    )
    half = ks // CORES
    steps = 4
    red_width = half // steps
    count = len(chunks)
    own = (n1 - 1) + (n2 - 1)
    diagonal = (n1 - 1) * (n2 - 1)
    n_sends = (
        count * (2 * own + 2 * diagonal + nchips) + 2 + (n - 1) + steps * (nchips - 1) + steps
    )
    line = jnp.pad(tw.reshape(1, tokens), ((0, 0), (0, width - tokens)))
    vmem, anywhere = pl.BlockSpec(memory_space=pltpu.VMEM), pl.BlockSpec(memory_space=pl.ANY)
    dma = pltpu.SemaphoreType.DMA
    bf16 = jnp.bfloat16
    kl, grad = pl.pallas_call(
        functools.partial(kernel, (n1, n2, chunks, red_width)),
        out_shape=(
            jax.ShapeDtypeStruct((1, rows), F32),
            jax.ShapeDtypeStruct((rows, ks), F32),
        ),
        in_specs=[anywhere, anywhere, vmem, anywhere, anywhere],
        out_specs=(vmem, vmem),
        scratch_shapes=[
            pltpu.VMEM((rows, kt), bf16),
            pltpu.VMEM((rows, ks), bf16),
            pltpu.VMEM((kt, cols), bf16),
            pltpu.VMEM((ks, cols), bf16),
            pltpu.VMEM((half, cols), bf16),
            pltpu.VMEM((n, PACK, td), bf16),
            pltpu.VMEM((n, PACK, sd), bf16),
            pltpu.VMEM((n * PACK, cols), F32),
            pltpu.VMEM((n * PACK, cols), F32),
            pltpu.VMEM((2, tokens, cols), F32),
            pltpu.VMEM((2, tokens, cols), F32),
            pltpu.VMEM((n, 8, width), F32),
            pltpu.VMEM((nchips, CORES * rows, half), F32),
            pltpu.VMEM((nchips, steps, PACK, red_width // 2), bf16),
            pltpu.VMEM((nchips, steps, PACK, red_width // 2), bf16),
            pltpu.VMEM((steps, CORES * rows, red_width), F32),
            pltpu.VMEM((steps, CORES * rows, red_width), F32),
            dma((2,)),
            dma((count, fold)),
            dma,
            dma((n_sends,)),
            dma((2 * count, n)),
            dma((count, n)),
            dma,
            dma((n,)),
            dma((nchips, steps)),
            dma((steps,)),
        ],
        compiler_params=pltpu.CompilerParams(
            collective_id=0, has_side_effects=True, vmem_limit_bytes=60 * 1024 * 1024
        ),
    )(th, sh, line, thead, shead)
    return kl.reshape(rows), grad


def solution(mesh):
    n1, n2 = mesh.shape["vocab"] // CORES, mesh.shape["section"]
    in_specs = (
        P(("dp", "vocab", "section"), None),
        P(("dp", "vocab", "section"), None),
        P(None, ("vocab", "section")),
        P(None, ("vocab", "section")),
        P("dp"),
    )
    out_specs = (P(("dp", "vocab", "section")), P(("dp", "vocab", "section"), None))
    return jax.shard_map(
        functools.partial(shards, n1, n2),
        mesh=mesh,
        in_specs=in_specs,
        out_specs=out_specs,
        check_vma=False,
    )
```

```python
import functools

import jax
import jax.numpy as jnp
from jax import lax
from jax.experimental import pallas as pl
from jax.experimental.pallas import tpu as pltpu
from jax.sharding import PartitionSpec as P

CORES = 2
PACK = 16
BLOCK = 8
F32 = jnp.float32


def kernel(
    dims,
    th_hbm,
    sh_hbm,
    tw_ref,
    thead_hbm,
    shead_hbm,
    kl_ref,
    grad_ref,
    th_in,
    sh_in,
    thead,
    shead,
    phead,
    gt,
    gs,
    acc_t,
    acc_s,
    logits,
    plogits,
    stats,
    part,
    sbuf,
    rbuf,
    in_sem,
    thead_sem,
    phead_sem,
    send_sem,
    piece_sem,
    pair_sem,
    logit_sem,
    stat_sem,
    red_sem,
):
    n1, n2, chunks, red_width = dims
    nchips = n1 * n2
    n = nchips * CORES
    rows, kt = th_in.shape
    ks = sh_in.shape[1]
    fold = PACK // rows
    tokens = n * rows
    pair_rows = CORES * rows
    half = ks // CORES
    width = stats.shape[2]

    position, s = lax.axis_index("vocab"), lax.axis_index("section")
    v, c = position // CORES, position % CORES
    other = 1 - c
    chip = v * n2 + s
    slot = chip * CORES + c

    def device(v, s, c):
        return {"vocab": v * CORES + c, "section": s}

    sends, early = [], []

    def push(src, dst, recv, target):
        copy = pltpu.make_async_remote_copy(
            src_ref=src,
            dst_ref=dst,
            send_sem=send_sem.at[len(sends)],
            recv_sem=recv,
            device_id=target,
            device_id_type=pl.DeviceIdType.MESH,
        )
        copy.start()
        sends.append(copy)

    def arrive(dst, recv):
        pltpu.make_async_remote_copy(
            src_ref=dst,
            dst_ref=dst,
            send_sem=send_sem.at[0],
            recv_sem=recv,
            device_id=device(v, s, other),
            device_id_type=pl.DeviceIdType.MESH,
        ).wait_recv()

    barrier = pltpu.get_barrier_semaphore()
    for dv in range(n1):
        for ds in range(n2):
            for dc in range(CORES):
                if dv or ds or dc:
                    pl.semaphore_signal(
                        barrier,
                        inc=1,
                        device_id=device((v + dv) % n1, (s + ds) % n2, (c + dc) % CORES),
                        device_id_type=pl.DeviceIdType.MESH,
                    )
    load_t = pltpu.make_async_copy(th_hbm, th_in, in_sem.at[0])
    load_s = pltpu.make_async_copy(sh_hbm, sh_in, in_sem.at[1])
    load_t.start()
    load_s.start()
    load_t.wait()
    load_s.wait()
    for src, dst in ((th_in, gt), (sh_in, gs)):
        depth = src.shape[1] // fold
        dst[slot] = jnp.concatenate(
            [src[:, q * depth : (q + 1) * depth] for q in range(fold)], axis=0
        )
    row = lax.broadcasted_iota(jnp.int32, (tokens, width), 0)
    lane = lax.broadcasted_iota(jnp.int32, (tokens, width), 1)
    eye = row == lane
    row_chip, row_core, row_token = row // pair_rows, row % pair_rows // rows, row % rows
    source = ((row_chip // n2 * CORES + row_core) * n2 + row_chip % n2) * rows + row_token
    weight = jnp.sum(
        jnp.where(
            source[:, :tokens] == lane[:, :tokens],
            jnp.broadcast_to(tw_ref[...], (tokens, tokens)),
            0.0,
        ),
        axis=1,
        keepdims=True,
    )
    pl.semaphore_wait(barrier, n - 1)

    def piece(index, where, h):
        is_teacher, first, size, _ = chunks[index]
        buf = gt if is_teacher else gs
        return buf.at[where, :, pl.ds(first + h * (size // 2), size // 2)]

    def whole(index, where):
        is_teacher, first, size, _ = chunks[index]
        buf = gt if is_teacher else gs
        return buf.at[where, :, pl.ds(first, size)]

    def slot_of(v, s, c):
        return (v * n2 + s) * CORES + c

    count = len(chunks)
    along_v = [(v + dv) % n1 for dv in range(1, n1)]
    along_s = [(s + ds) % n2 for ds in range(1, n2)]
    for turn in range(2):
        begun = len(sends)
        for i in range(count):
            for h, targets in (
                (turn, [device(to, s, c) for to in along_v]),
                (1 - turn, [device(v, to, c) for to in along_s]),
            ):
                ref, sem = piece(i, slot, h), piece_sem.at[2 * i + h, slot]
                for target in targets:
                    push(ref, ref, sem, target)
        if turn == 0:
            for copy in sends[begun:]:
                early.append(copy)
            loads = {}
            for index, (is_teacher, first, size, _) in enumerate(chunks):
                src, dst = (thead_hbm, thead) if is_teacher else (shead_hbm, shead)
                depth = (kt if is_teacher else ks) // fold
                for q in range(fold):
                    span = pl.ds(q * depth + first, size)
                    copy = pltpu.make_async_copy(src.at[span], dst.at[span], thead_sem.at[index, q])
                    copy.start()
                    loads[index, q] = copy
            for i in range(count):
                push(whole(i, slot), whole(i, slot), pair_sem.at[i, slot], device(v, s, other))
            push(
                shead_hbm.at[pl.ds(pl.multiple_of(other * half, half), half)],
                phead,
                phead_sem,
                device(v, s, other),
            )
            for copy in early:
                copy.wait_send()
    for turn in range(2):
        for i in range(count):
            for frm in along_v:
                at = slot_of(frm, s, c)
                ref, sem = piece(i, at, turn), piece_sem.at[2 * i + turn, at]
                arrive(ref, sem)
                if turn == 0:
                    for to in along_s:
                        push(ref, ref, sem, device(v, to, c))
            for frm in along_s:
                at = slot_of(v, frm, c)
                ref, sem = piece(i, at, 1 - turn), piece_sem.at[2 * i + 1 - turn, at]
                arrive(ref, sem)
                if turn == 0:
                    for to in along_v:
                        push(ref, ref, sem, device(to, s, c))
            if turn == 1:
                for at in [slot_of(frm, s, c) for frm in along_v] + [
                    slot_of(v, frm, c) for frm in along_s
                ]:
                    push(whole(i, at), whole(i, at), pair_sem.at[i, at], device(v, s, other))

    block = min(BLOCK, n)
    row_part = lax.broadcasted_iota(jnp.int32, (block * PACK, acc_t.shape[1]), 0) % PACK // rows
    for i in range(count):
        for fv in along_v:
            for fs in along_s:
                at = slot_of(fv, fs, c)
                for h in range(2):
                    arrive(piece(i, at, h), piece_sem.at[2 * i + h, at])
                push(whole(i, at), whole(i, at), pair_sem.at[i, at], device(v, s, other))
        for fv in range(n1):
            for fs in range(n2):
                at = slot_of((v + fv) % n1, (s + fs) % n2, other)
                arrive(whole(i, at), pair_sem.at[i, at])
        for q in range(fold):
            loads[i, q].wait()
        is_teacher, first, size, fresh = chunks[i]
        buf, head, acc = (gt, thead, acc_t) if is_teacher else (gs, shead, acc_s)
        depth = (kt if is_teacher else ks) // fold

        def multiply(b):
            lhs = buf[pl.ds(b * block, block), :, first : first + size].reshape(block * PACK, size)
            total = None
            for q in range(fold):
                rhs = head[q * depth + first : q * depth + first + size, :]
                product = jnp.dot(lhs, rhs, preferred_element_type=F32)
                total = product if total is None else jnp.where(row_part == q, product, total)
            where = pl.ds(b * block * PACK, block * PACK)
            acc[where, :] = total if fresh else acc[where, :] + total

        if n > block:
            pl.loop(0, n // block)(multiply)
        else:
            multiply(0)

    def compact(acc):
        cols = acc.shape[1]
        x = acc[...].reshape(n, PACK // 8, 8, cols)
        total = x[:, 0] + x[:, 1]
        total = total + jnp.concatenate([total[:, rows:], total[:, :rows]], axis=1)
        total = total.reshape(nchips, CORES, 8, cols)
        sub = lax.broadcasted_iota(jnp.int32, (nchips, 8, cols), 1)
        return jnp.where(sub < rows, total[:, 0], total[:, 1]).reshape(tokens, cols)

    tl, sl = compact(acc_t), compact(acc_s)
    logits[0] = tl
    logits[1] = sl
    push(logits, plogits, logit_sem, device(v, s, other))
    tmax = jnp.max(tl, axis=1, keepdims=True)
    smax = jnp.max(sl, axis=1, keepdims=True)
    texp = jnp.exp(tl - tmax)
    columns = (
        tmax,
        smax,
        jnp.sum(texp, axis=1, keepdims=True),
        jnp.sum(jnp.exp(sl - smax), axis=1, keepdims=True),
        jnp.sum(texp * (tl - sl), axis=1, keepdims=True),
    )
    lines = [jnp.sum(jnp.where(eye, col, 0.0), axis=0, keepdims=True) for col in columns]
    lines.append(jnp.zeros((8 - len(lines), width), F32))
    stats[slot] = jnp.concatenate(lines, axis=0)
    for dv in reversed(range(n1)):
        for ds in reversed(range(n2)):
            for dc in range(CORES):
                if dv or ds or dc:
                    to = device((v + dv) % n1, (s + ds) % n2, (c + dc) % CORES)
                    push(stats.at[slot], stats.at[slot], stat_sem.at[slot], to)
    for dv in range(n1):
        for ds in range(n2):
            for dc in range(CORES):
                if dv or ds or dc:
                    at = slot_of((v + dv) % n1, (s + ds) % n2, (c + dc) % CORES)
                    arrive(stats.at[at], stat_sem.at[at])
    arrive(plogits, logit_sem)
    arrive(phead, phead_sem)
    allstats = stats[...]
    tm, sm = allstats[:, 0], allstats[:, 1]
    tmax = jnp.max(tm, axis=0, keepdims=True)
    smax = jnp.max(sm, axis=0, keepdims=True)
    tscale = jnp.exp(tm - tmax)
    ttotal = jnp.sum(allstats[:, 2] * tscale, axis=0, keepdims=True)
    stotal = jnp.sum(allstats[:, 3] * jnp.exp(sm - smax), axis=0, keepdims=True)
    cross = jnp.sum(allstats[:, 4] * tscale, axis=0, keepdims=True)
    tlse = tmax + jnp.log(ttotal)
    slse = smax + jnp.log(stotal)
    kl = cross / ttotal - tlse + slse

    def column(line):
        return jnp.sum(
            jnp.where(eye, jnp.broadcast_to(line, (tokens, width)), 0.0), axis=1, keepdims=True
        )

    tlse, slse = column(tlse), column(slse)
    grads = []
    for ref in (logits, plogits):
        diff = jnp.exp(ref[1] - slse) - jnp.exp(ref[0] - tlse)
        grads.append((weight * diff).astype(jnp.bfloat16))

    steps = half // red_width
    narrow = red_width // fold

    def fold_rows(x):
        return jnp.concatenate(
            [x[:, :, q * narrow : (q + 1) * narrow] for q in range(fold)], axis=1
        )

    nt = (((1,), (1,)), ((), ()))
    for j in range(steps):
        mine = pl.ds(pl.multiple_of(c * half + j * red_width, red_width), red_width)
        total = lax.dot_general(grads[0], shead[mine, :], nt, preferred_element_type=F32)
        total += lax.dot_general(
            grads[1],
            phead[j * red_width : (j + 1) * red_width, :],
            nt,
            preferred_element_type=F32,
        )
        total = total.reshape(nchips, pair_rows, red_width)
        packed = [fold_rows(total[:, d * rows : (d + 1) * rows]) for d in range(CORES)]
        part[:, j] = jnp.where(c == 0, packed[0], packed[1])
        for d in range(CORES):
            sbuf[:, d, j] = packed[d].astype(jnp.bfloat16)
        for dv in reversed(range(n1)):
            for ds in reversed(range(n2)):
                for d in (c, other):
                    if dv or ds or d is other:
                        tv, ts = (v + dv) % n1, (s + ds) % n2
                        push(
                            sbuf.at[tv * n2 + ts, d, j],
                            rbuf.at[slot, j],
                            red_sem.at[slot, j],
                            device(tv, ts, d),
                        )

    kl_rows = column(kl)
    kl_ref[...] = jnp.sum(jnp.where(row == slot * rows + lane, kl_rows, 0.0), axis=0, keepdims=True)[
        :, :rows
    ]

    for j in range(steps):
        for d in (c, other):
            total = part[chip, j] if d is c else None
            for dv in range(n1):
                for ds in range(n2):
                    if dv or ds or d is other:
                        at = slot_of((v + dv) % n1, (s + ds) % n2, d)
                        arrive(rbuf.at[at, j], red_sem.at[at, j])
                        got = rbuf[at, j].astype(F32)
                        total = got if total is None else total + got
            for q in range(fold):
                to = pl.multiple_of(d * half + j * red_width + q * narrow, narrow)
                grad_ref[:, pl.ds(to, narrow)] = total[q * rows : (q + 1) * rows]
    for copy in sends:
        if not any(copy is done for done in early):
            copy.wait_send()


def deliver(kl_in, grad_in, kl_ref, grad_ref):
    kl_ref[...] = kl_in[...]
    grad_ref[...] = grad_in[...]


def shards(n1, n2, th, sh, thead, shead, tw):
    nchips = n1 * n2
    n = nchips * CORES
    rows, kt = th.shape
    ks = sh.shape[1]
    cols = thead.shape[1]
    fold = PACK // rows
    tokens = n * rows
    width = -(-tokens // 128) * 128
    td, sd = kt // fold, ks // fold
    chunks = (
        (True, 0, td // 2, True),
        (True, td // 2, td // 2, False),
        (False, 0, sd, True),
    )
    half = ks // CORES
    steps = 4
    red_width = half // steps
    count = len(chunks)
    own = (n1 - 1) + (n2 - 1)
    diagonal = (n1 - 1) * (n2 - 1)
    n_sends = (
        count * (2 * own + 2 * diagonal + nchips) + 2 + (n - 1) + steps * (n - 1)
    )
    line = tw.reshape(1, tokens)
    vmem, anywhere = pl.BlockSpec(memory_space=pltpu.VMEM), pl.BlockSpec(memory_space=pltpu.HBM)
    dma = pltpu.SemaphoreType.DMA
    bf16 = jnp.bfloat16
    kl, grad = pl.pallas_call(
        functools.partial(kernel, (n1, n2, chunks, red_width)),
        out_shape=(
            jax.ShapeDtypeStruct((1, rows), F32),
            jax.ShapeDtypeStruct((rows, ks), F32),
        ),
        in_specs=[anywhere, anywhere, vmem, anywhere, anywhere],
        out_specs=(vmem, vmem),
        scratch_shapes=[
            pltpu.VMEM((rows, kt), bf16),
            pltpu.VMEM((rows, ks), bf16),
            pltpu.VMEM((kt, cols), bf16),
            pltpu.VMEM((ks, cols), bf16),
            pltpu.VMEM((half, cols), bf16),
            pltpu.VMEM((n, PACK, td), bf16),
            pltpu.VMEM((n, PACK, sd), bf16),
            pltpu.VMEM((n * PACK, cols), F32),
            pltpu.VMEM((n * PACK, cols), F32),
            pltpu.VMEM((2, tokens, cols), F32),
            pltpu.VMEM((2, tokens, cols), F32),
            pltpu.VMEM((n, 8, width), F32),
            pltpu.VMEM((nchips, steps, PACK, red_width // fold), F32),
            pltpu.VMEM((nchips, CORES, steps, PACK, red_width // fold), bf16),
            pltpu.VMEM((n, steps, PACK, red_width // fold), bf16),
            dma((2,)),
            dma((count, fold)),
            dma,
            dma((n_sends,)),
            dma((2 * count, n)),
            dma((count, n)),
            dma,
            dma((n,)),
            dma((n, steps)),
        ],
        compiler_params=pltpu.CompilerParams(
            collective_id=0, has_side_effects=True, vmem_limit_bytes=60 * 1024 * 1024
        ),
    )(th, sh, line, thead, shead)
    kl, grad = pl.pallas_call(
        deliver,
        out_shape=(
            jax.ShapeDtypeStruct((1, rows), F32),
            jax.ShapeDtypeStruct((rows, ks), F32),
        ),
        in_specs=[vmem, vmem],
        out_specs=(vmem, vmem),
    )(kl, grad)
    return kl.reshape(rows), grad


def solution(mesh):
    n1, n2 = mesh.shape["vocab"] // CORES, mesh.shape["section"]
    in_specs = (
        P(("dp", "vocab", "section"), None),
        P(("dp", "vocab", "section"), None),
        P(None, ("vocab", "section")),
        P(None, ("vocab", "section")),
        P("dp"),
    )
    out_specs = (P(("dp", "vocab", "section")), P(("dp", "vocab", "section"), None))
    return jax.shard_map(
        functools.partial(shards, n1, n2),
        mesh=mesh,
        in_specs=in_specs,
        out_specs=out_specs,
        check_vma=False,
    )
```

```python
import functools

import jax
import jax.numpy as jnp
from jax import lax
from jax.experimental import pallas as pl
from jax.experimental.pallas import tpu as pltpu
from jax.sharding import PartitionSpec as P

CORES = 2
PACK = 16
BLOCK = 8
F32 = jnp.float32


def kernel(
    dims,
    th_hbm,
    sh_hbm,
    tw_ref,
    thead_hbm,
    shead_hbm,
    kl_ref,
    grad_ref,
    th_in,
    sh_in,
    thead,
    shead,
    phead,
    gt,
    gs,
    acc_t,
    acc_s,
    logits,
    plogits,
    stats,
    part,
    sbuf,
    rbuf,
    in_sem,
    thead_sem,
    phead_sem,
    send_sem,
    piece_sem,
    pair_sem,
    logit_sem,
    stat_sem,
    red_sem,
):
    n1, n2, chunks, red_width = dims
    nchips = n1 * n2
    n = nchips * CORES
    rows, kt = th_in.shape
    ks = sh_in.shape[1]
    fold = PACK // rows
    tokens = n * rows
    pair_rows = CORES * rows
    half = ks // CORES
    width = stats.shape[2]

    position, s = lax.axis_index("vocab"), lax.axis_index("section")
    v, c = position // CORES, position % CORES
    other = 1 - c
    chip = v * n2 + s
    slot = chip * CORES + c

    def device(v, s, c):
        return {"vocab": v * CORES + c, "section": s}

    sends, early = [], []

    def push(src, dst, recv, target):
        copy = pltpu.make_async_remote_copy(
            src_ref=src,
            dst_ref=dst,
            send_sem=send_sem.at[len(sends)],
            recv_sem=recv,
            device_id=target,
            device_id_type=pl.DeviceIdType.MESH,
        )
        copy.start()
        sends.append(copy)

    def arrive(dst, recv):
        pltpu.make_async_remote_copy(
            src_ref=dst,
            dst_ref=dst,
            send_sem=send_sem.at[0],
            recv_sem=recv,
            device_id=device(v, s, other),
            device_id_type=pl.DeviceIdType.MESH,
        ).wait_recv()

    barrier = pltpu.get_barrier_semaphore()
    for dv in range(n1):
        for ds in range(n2):
            for dc in range(CORES):
                if dv or ds or dc:
                    pl.semaphore_signal(
                        barrier,
                        inc=1,
                        device_id=device((v + dv) % n1, (s + ds) % n2, (c + dc) % CORES),
                        device_id_type=pl.DeviceIdType.MESH,
                    )
    load_t = pltpu.make_async_copy(th_hbm, th_in, in_sem.at[0])
    load_s = pltpu.make_async_copy(sh_hbm, sh_in, in_sem.at[1])
    load_t.start()
    load_s.start()
    load_t.wait()
    load_s.wait()
    for src, dst in ((th_in, gt), (sh_in, gs)):
        depth = src.shape[1] // fold
        dst[slot] = jnp.concatenate(
            [src[:, q * depth : (q + 1) * depth] for q in range(fold)], axis=0
        )
    row = lax.broadcasted_iota(jnp.int32, (tokens, width), 0)
    lane = lax.broadcasted_iota(jnp.int32, (tokens, width), 1)
    eye = row == lane
    row_chip, row_core, row_token = row // pair_rows, row % pair_rows // rows, row % rows
    source = ((row_chip // n2 * CORES + row_core) * n2 + row_chip % n2) * rows + row_token
    weight = jnp.sum(
        jnp.where(
            source[:, :tokens] == lane[:, :tokens],
            jnp.broadcast_to(tw_ref[...], (tokens, tokens)),
            0.0,
        ),
        axis=1,
        keepdims=True,
    )
    pl.semaphore_wait(barrier, n - 1)

    def piece(index, where, h):
        is_teacher, first, size, _ = chunks[index]
        buf = gt if is_teacher else gs
        return buf.at[where, :, pl.ds(first + h * (size // 2), size // 2)]

    def whole(index, where):
        is_teacher, first, size, _ = chunks[index]
        buf = gt if is_teacher else gs
        return buf.at[where, :, pl.ds(first, size)]

    def slot_of(v, s, c):
        return (v * n2 + s) * CORES + c

    count = len(chunks)
    along_v = [(v + dv) % n1 for dv in range(1, n1)]
    along_s = [(s + ds) % n2 for ds in range(1, n2)]
    for turn in range(2):
        begun = len(sends)
        for i in range(count):
            for h, targets in (
                (turn, [device(to, s, c) for to in along_v]),
                (1 - turn, [device(v, to, c) for to in along_s]),
            ):
                ref, sem = piece(i, slot, h), piece_sem.at[2 * i + h, slot]
                for target in targets:
                    push(ref, ref, sem, target)
        if turn == 0:
            for copy in sends[begun:]:
                early.append(copy)
            loads = {}
            for index, (is_teacher, first, size, _) in enumerate(chunks):
                src, dst = (thead_hbm, thead) if is_teacher else (shead_hbm, shead)
                depth = (kt if is_teacher else ks) // fold
                for q in range(fold):
                    span = pl.ds(q * depth + first, size)
                    copy = pltpu.make_async_copy(src.at[span], dst.at[span], thead_sem.at[index, q])
                    copy.start()
                    loads[index, q] = copy
            for i in range(count):
                push(whole(i, slot), whole(i, slot), pair_sem.at[i, slot], device(v, s, other))
            push(
                shead_hbm.at[pl.ds(pl.multiple_of(other * half, half), half)],
                phead,
                phead_sem,
                device(v, s, other),
            )
            for copy in early:
                copy.wait_send()
    for turn in range(2):
        for i in range(count):
            for frm in along_v:
                at = slot_of(frm, s, c)
                ref, sem = piece(i, at, turn), piece_sem.at[2 * i + turn, at]
                arrive(ref, sem)
                if turn == 0:
                    for to in along_s:
                        push(ref, ref, sem, device(v, to, c))
            for frm in along_s:
                at = slot_of(v, frm, c)
                ref, sem = piece(i, at, 1 - turn), piece_sem.at[2 * i + 1 - turn, at]
                arrive(ref, sem)
                if turn == 0:
                    for to in along_v:
                        push(ref, ref, sem, device(to, s, c))
            if turn == 1:
                for at in [slot_of(frm, s, c) for frm in along_v] + [
                    slot_of(v, frm, c) for frm in along_s
                ]:
                    push(whole(i, at), whole(i, at), pair_sem.at[i, at], device(v, s, other))

    block = min(BLOCK, n)
    row_part = lax.broadcasted_iota(jnp.int32, (block * PACK, acc_t.shape[1]), 0) % PACK // rows
    for i in range(count):
        for fv in along_v:
            for fs in along_s:
                at = slot_of(fv, fs, c)
                for h in range(2):
                    arrive(piece(i, at, h), piece_sem.at[2 * i + h, at])
                push(whole(i, at), whole(i, at), pair_sem.at[i, at], device(v, s, other))
        for fv in range(n1):
            for fs in range(n2):
                at = slot_of((v + fv) % n1, (s + fs) % n2, other)
                arrive(whole(i, at), pair_sem.at[i, at])
        for q in range(fold):
            loads[i, q].wait()
        is_teacher, first, size, fresh = chunks[i]
        buf, head, acc = (gt, thead, acc_t) if is_teacher else (gs, shead, acc_s)
        depth = (kt if is_teacher else ks) // fold

        def multiply(b):
            lhs = buf[pl.ds(b * block, block), :, first : first + size].reshape(block * PACK, size)
            total = None
            for q in range(fold):
                rhs = head[q * depth + first : q * depth + first + size, :]
                product = jnp.dot(lhs, rhs, preferred_element_type=F32)
                total = product if total is None else jnp.where(row_part == q, product, total)
            where = pl.ds(b * block * PACK, block * PACK)
            acc[where, :] = total if fresh else acc[where, :] + total

        if n > block:
            pl.loop(0, n // block)(multiply)
        else:
            multiply(0)

    def compact(acc):
        cols = acc.shape[1]
        x = acc[...].reshape(n, PACK // 8, 8, cols)
        total = x[:, 0] + x[:, 1]
        total = total + jnp.concatenate([total[:, rows:], total[:, :rows]], axis=1)
        total = total.reshape(nchips, CORES, 8, cols)
        sub = lax.broadcasted_iota(jnp.int32, (nchips, 8, cols), 1)
        return jnp.where(sub < rows, total[:, 0], total[:, 1]).reshape(tokens, cols)

    tl, sl = compact(acc_t), compact(acc_s)
    logits[0] = tl
    logits[1] = sl
    push(logits, plogits, logit_sem, device(v, s, other))
    tmax = jnp.max(tl, axis=1, keepdims=True)
    smax = jnp.max(sl, axis=1, keepdims=True)
    texp = jnp.exp(tl - tmax)
    columns = (
        tmax,
        smax,
        jnp.sum(texp, axis=1, keepdims=True),
        jnp.sum(jnp.exp(sl - smax), axis=1, keepdims=True),
        jnp.sum(texp * (tl - sl), axis=1, keepdims=True),
    )
    lines = [jnp.sum(jnp.where(eye, col, 0.0), axis=0, keepdims=True) for col in columns]
    lines.append(jnp.zeros((8 - len(lines), width), F32))
    stats[slot] = jnp.concatenate(lines, axis=0)
    for dv in reversed(range(n1)):
        for ds in reversed(range(n2)):
            for dc in range(CORES):
                if dv or ds or dc:
                    to = device((v + dv) % n1, (s + ds) % n2, (c + dc) % CORES)
                    push(stats.at[slot], stats.at[slot], stat_sem.at[slot], to)
    for dv in range(n1):
        for ds in range(n2):
            for dc in range(CORES):
                if dv or ds or dc:
                    at = slot_of((v + dv) % n1, (s + ds) % n2, (c + dc) % CORES)
                    arrive(stats.at[at], stat_sem.at[at])
    arrive(plogits, logit_sem)
    arrive(phead, phead_sem)
    allstats = stats[...]
    tm, sm = allstats[:, 0], allstats[:, 1]
    tmax = jnp.max(tm, axis=0, keepdims=True)
    smax = jnp.max(sm, axis=0, keepdims=True)
    tscale = jnp.exp(tm - tmax)
    ttotal = jnp.sum(allstats[:, 2] * tscale, axis=0, keepdims=True)
    stotal = jnp.sum(allstats[:, 3] * jnp.exp(sm - smax), axis=0, keepdims=True)
    cross = jnp.sum(allstats[:, 4] * tscale, axis=0, keepdims=True)
    tlse = tmax + jnp.log(ttotal)
    slse = smax + jnp.log(stotal)
    kl = cross / ttotal - tlse + slse

    def column(line):
        return jnp.sum(
            jnp.where(eye, jnp.broadcast_to(line, (tokens, width)), 0.0), axis=1, keepdims=True
        )

    tlse, slse = column(tlse), column(slse)
    grads = []
    for ref in (logits, plogits):
        diff = jnp.exp(ref[1] - slse) - jnp.exp(ref[0] - tlse)
        grads.append((weight * diff).astype(jnp.bfloat16))

    steps = half // red_width
    narrow = red_width // fold

    def fold_rows(x):
        return jnp.concatenate(
            [x[:, :, q * narrow : (q + 1) * narrow] for q in range(fold)], axis=1
        )

    nt = (((1,), (1,)), ((), ()))
    for j in range(steps):
        mine = pl.ds(pl.multiple_of(c * half + j * red_width, red_width), red_width)
        total = lax.dot_general(grads[0], shead[mine, :], nt, preferred_element_type=F32)
        total += lax.dot_general(
            grads[1],
            phead[j * red_width : (j + 1) * red_width, :],
            nt,
            preferred_element_type=F32,
        )
        total = total.reshape(nchips, pair_rows, red_width)
        packed = [fold_rows(total[:, d * rows : (d + 1) * rows]) for d in range(CORES)]
        part[:, j] = jnp.where(c == 0, packed[0], packed[1])
        for d in range(CORES):
            sbuf[:, d, j] = packed[d].astype(jnp.bfloat16)
        for dv in reversed(range(n1)):
            for ds in reversed(range(n2)):
                for d in (c, other):
                    if dv or ds or d is other:
                        tv, ts = (v + dv) % n1, (s + ds) % n2
                        push(
                            sbuf.at[tv * n2 + ts, d, j],
                            rbuf.at[slot, j],
                            red_sem.at[slot, j],
                            device(tv, ts, d),
                        )

    kl_rows = column(kl)
    kl_ref[...] = jnp.sum(jnp.where(row == slot * rows + lane, kl_rows, 0.0), axis=0, keepdims=True)[
        :, :rows
    ]

    for j in range(steps):
        for d in (c, other):
            total = part[chip, j] if d is c else None
            for dv in range(n1):
                for ds in range(n2):
                    if dv or ds or d is other:
                        at = slot_of((v + dv) % n1, (s + ds) % n2, d)
                        arrive(rbuf.at[at, j], red_sem.at[at, j])
                        got = rbuf[at, j].astype(F32)
                        total = got if total is None else total + got
            for q in range(fold):
                to = pl.multiple_of(d * half + j * red_width + q * narrow, narrow)
                grad_ref[:, pl.ds(to, narrow)] = total[q * rows : (q + 1) * rows]
    for copy in sends:
        if not any(copy is done for done in early):
            copy.wait_send()


def deliver(kl_in, grad_in, kl_ref, grad_ref):
    kl_ref[...] = kl_in[...]
    grad_ref[...] = grad_in[...]


def shards(n1, n2, th, sh, thead, shead, tw):
    nchips = n1 * n2
    n = nchips * CORES
    rows, kt = th.shape
    ks = sh.shape[1]
    cols = thead.shape[1]
    fold = PACK // rows
    tokens = n * rows
    width = -(-tokens // 128) * 128
    td, sd = kt // fold, ks // fold
    chunks = (
        (True, 0, td // 2, True),
        (True, td // 2, td // 2, False),
        (False, 0, sd, True),
    )
    half = ks // CORES
    steps = 2
    red_width = half // steps
    count = len(chunks)
    own = (n1 - 1) + (n2 - 1)
    diagonal = (n1 - 1) * (n2 - 1)
    n_sends = (
        count * (2 * own + 2 * diagonal + nchips) + 2 + (n - 1) + steps * (n - 1)
    )
    line = tw.reshape(1, tokens)
    vmem, anywhere = pl.BlockSpec(memory_space=pltpu.VMEM), pl.BlockSpec(memory_space=pltpu.HBM)
    dma = pltpu.SemaphoreType.DMA
    bf16 = jnp.bfloat16
    kl, grad = pl.pallas_call(
        functools.partial(kernel, (n1, n2, chunks, red_width)),
        out_shape=(pltpu.VMEM((1, rows), F32), pltpu.VMEM((rows, ks), F32)),
        in_specs=[anywhere, anywhere, vmem, anywhere, anywhere],
        out_specs=(vmem, vmem),
        scratch_shapes=[
            pltpu.VMEM((rows, kt), bf16),
            pltpu.VMEM((rows, ks), bf16),
            pltpu.VMEM((kt, cols), bf16),
            pltpu.VMEM((ks, cols), bf16),
            pltpu.VMEM((half, cols), bf16),
            pltpu.VMEM((n, PACK, td), bf16),
            pltpu.VMEM((n, PACK, sd), bf16),
            pltpu.VMEM((n * PACK, cols), F32),
            pltpu.VMEM((n * PACK, cols), F32),
            pltpu.VMEM((2, tokens, cols), F32),
            pltpu.VMEM((2, tokens, cols), F32),
            pltpu.VMEM((n, 8, width), F32),
            pltpu.VMEM((nchips, steps, PACK, red_width // fold), F32),
            pltpu.VMEM((nchips, CORES, steps, PACK, red_width // fold), bf16),
            pltpu.VMEM((n, steps, PACK, red_width // fold), bf16),
            dma((2,)),
            dma((count, fold)),
            dma,
            dma((n_sends,)),
            dma((2 * count, n)),
            dma((count, n)),
            dma,
            dma((n,)),
            dma((n, steps)),
        ],
        compiler_params=pltpu.CompilerParams(
            collective_id=0, has_side_effects=True, vmem_limit_bytes=60 * 1024 * 1024
        ),
    )(th, sh, line, thead, shead)
    kl, grad = pl.pallas_call(
        deliver,
        out_shape=(
            jax.ShapeDtypeStruct((1, rows), F32),
            jax.ShapeDtypeStruct((rows, ks), F32),
        ),
        in_specs=[vmem, vmem],
        out_specs=(vmem, vmem),
        compiler_params=pltpu.CompilerParams(vmem_limit_bytes=4 * 1024 * 1024),
    )(kl, grad)
    return kl.reshape(rows), grad


def solution(mesh):
    n1, n2 = mesh.shape["vocab"] // CORES, mesh.shape["section"]
    in_specs = (
        P(("dp", "vocab", "section"), None),
        P(("dp", "vocab", "section"), None),
        P(None, ("vocab", "section")),
        P(None, ("vocab", "section")),
        P("dp"),
    )
    out_specs = (P(("dp", "vocab", "section")), P(("dp", "vocab", "section"), None))
    return jax.shard_map(
        functools.partial(shards, n1, n2),
        mesh=mesh,
        in_specs=in_specs,
        out_specs=out_specs,
        check_vma=False,
    )
```
